32 devices in a mesh: band: 8 (over y, x, core), sub: 4 (over z).
Axes of the slice: x: 2, y: 2, z: 4, core: 2. Of those that a mesh axis runs over, the one named last changes fastest.
Arguments:
- gas_amounts: bfloat16 [512, 64, 8, 128], P('band'), may hold values from 0.049804688 to 1
- layer_mass: bfloat16 [512, 64, 128], P('band'), may hold values from 4 to 40
- column_state: bfloat16 [512, 2, 128], P('band'), may hold values from 0.099609375 to 0.796875
- absorption: bfloat16 [112, 8], P('sub'), may hold values from 0.0019989014 to 0.5
- single_scatter: float32 [112], P('sub'), may hold values from 0.2 to 0.95
- solar_weight: float32 [112], P('sub'), may hold values from 0.002 to 0.1
- sunlit: int32 [512], replicated, may hold values from 0 to 1, as said below
Outputs:
- heating: float32 [512, 64, 128], P(('band', 'sub'))
- surface_down: float32 [512, 128], P(('band', 'sub'))
The draws below stay inside these ranges and needn't reach their ends.
Inputs may be any that keep to these rules, and one draw needn't show every extreme that they name: Exactly 256 blocks are sunlit, and in every draw all 64 blocks of some band index are sunlit.
All inputs are finite; a program needn't handle non-finite values.
Results may differ from the reference program's by a relative error of at most 0.0003.
Values may be sent and summed in bfloat16 or wider, within the bound.
A program may use at most 256 MiB of HBM per device.

```python
import math
import jax
import jax.numpy as jnp
from jax import lax

LEVELS = 64
GPOINTS = 112
GASES = 8
BLOCK_COLS = 128
BLK_DEV = 64
BLOCKS = 512


def draw_sunlit(key, part):
    base = jax.random.fold_in(key, 17)
    key_shift, key_noise, key_top = jax.random.split(base, 3)
    band_total = BLOCKS // BLK_DEV
    shifts = jax.random.randint(key_shift, (band_total,), 0, 4).astype(jnp.int32)
    chosen = jax.random.randint(key_top, (), 0, band_total).astype(jnp.int32)
    shifts = shifts + jnp.where(jnp.arange(band_total, dtype=jnp.int32) == chosen, 8, 0).astype(jnp.int32)
    noise = jax.random.randint(key_noise, (BLOCKS,), 0, 65536).astype(jnp.int32)
    scores = (jnp.repeat(shifts, BLK_DEV) * 65536 + noise) * BLOCKS + jnp.arange(BLOCKS, dtype=jnp.int32)
    _, picked = lax.top_k(scores, BLOCKS // 2)
    return jnp.zeros((BLOCKS,), jnp.int32).at[picked].set(1)


def block_scale(own_key, extent, pieces, smallest, largest):
    def one(position, blocks):
        draws = jax.random.uniform(jax.random.fold_in(jax.random.fold_in(own_key, 6), position), (blocks,), jnp.float32, smallest / len(pieces), largest / len(pieces))
        return jnp.repeat(jnp.exp(draws), extent[position] // blocks).reshape((-1,) + (1,) * (len(extent) - position - 1))

    factor_of = one(*pieces[0])
    for cut in pieces[1:]:
        factor_of = factor_of * one(*cut)
    return factor_of


def setup_inputs(seed: int = 0) -> dict:
    key_of = jax.random.split(jax.random.key(seed), 8)
    gas_amounts = jnp.clip(jnp.exp(math.log(1.0) - 2.9996462 * jax.random.uniform(key_of[0], (BLOCKS, LEVELS, GASES, BLOCK_COLS), jnp.float32) ** block_scale(key_of[0], (BLOCKS, LEVELS, GASES, BLOCK_COLS), ((0, 8),), -0.2, 0.2)), 0.049804688, 1.0).astype(jnp.bfloat16)
    layer_mass = jnp.clip(jnp.exp(math.log(40.0) - 2.3025851 * jax.random.uniform(key_of[1], (BLOCKS, LEVELS, BLOCK_COLS), jnp.float32) ** block_scale(key_of[1], (BLOCKS, LEVELS, BLOCK_COLS), ((0, 8),), -0.2, 0.2)), 4.0, 40.0).astype(jnp.bfloat16)
    column_state = jnp.clip(0.099609375 + 0.6972656 * jax.random.uniform(key_of[2], (BLOCKS, 2, BLOCK_COLS), jnp.float32) ** block_scale(key_of[2], (BLOCKS, 2, BLOCK_COLS), ((0, 8),), -0.2, 0.2), 0.099609375, 0.796875).astype(jnp.bfloat16)
    absorption = jnp.clip(jnp.exp(math.log(0.5) - 5.5220104 * jax.random.uniform(key_of[3], (GPOINTS, GASES), jnp.float32) ** block_scale(key_of[3], (GPOINTS, GASES), ((0, 4),), -0.2, 0.2)), 0.0019989014, 0.5).astype(jnp.bfloat16)
    single_scatter = jnp.clip(0.2 + 0.75 * jax.random.uniform(key_of[4], (GPOINTS,), jnp.float32) ** block_scale(key_of[4], (GPOINTS,), ((0, 4),), -0.2, 0.2), 0.2, 0.95)
    solar_weight = jnp.clip(jnp.exp(math.log(0.1) - 3.912023 * jax.random.uniform(key_of[5], (GPOINTS,), jnp.float32) ** block_scale(key_of[5], (GPOINTS,), ((0, 4),), -0.2, 0.2)), 0.002, 0.1)
    sunlit = draw_sunlit(jax.random.fold_in(key_of[7], 71), 0)
    return dict(gas_amounts=gas_amounts, layer_mass=layer_mass, column_state=column_state, absorption=absorption, single_scatter=single_scatter, solar_weight=solar_weight, sunlit=sunlit)


def layer_solve(optical, heat_factor, cosine, ground, single_scatter, solar_weight):
    omega = single_scatter[:, None]
    passing = jnp.exp(-optical)
    reflected = 0.5 * omega * (1.0 - passing * passing)
    unscattered = jnp.exp(-optical / cosine[None, None, :])

    def upward(lower_albedo, layer_data):
        reflect_now, pass_now = layer_data
        denominator = 1.0 - reflect_now * lower_albedo
        upper_albedo = reflect_now + pass_now * pass_now * lower_albedo / denominator
        return upper_albedo, (upper_albedo, denominator)

    surface = jnp.broadcast_to(ground[None, :], optical.shape[1:])
    _, (stack_albedo, denominators) = lax.scan(upward, surface, (reflected, passing), reverse=True, unroll=8)

    def downward(state_now, layer_data):
        beam, diffuse = state_now
        albedo_now, pass_now, direct_now, denominator = layer_data
        net_flux = (1.0 - albedo_now) * (beam + diffuse)
        new_beam = beam * direct_now
        new_diffuse = (pass_now * diffuse + 0.5 * omega * (1.0 - direct_now) * beam) / denominator
        return (new_beam, new_diffuse), jnp.sum(net_flux, axis=0)

    top_beam = solar_weight[:, None] * cosine[None, :]
    (beam, diffuse), net_sums = lax.scan(downward, (top_beam, jnp.zeros_like(top_beam)), (stack_albedo, passing, unscattered, denominators), unroll=8)
    bottom_down = beam + diffuse
    bottom_net = jnp.sum((1.0 - ground[None, :]) * bottom_down, axis=0)
    interfaces = jnp.concatenate([net_sums, bottom_net[None, :]], axis=0)
    heating = heat_factor * (interfaces[:-1] - interfaces[1:])
    return heating, jnp.sum(bottom_down, axis=0)


def reference(gas_amounts, layer_mass, column_state, absorption, single_scatter, solar_weight, sunlit):
    coefficients = absorption.astype(jnp.float32)

    def one_block(block_data):
        block_gas, block_mass, block_state, block_flag = block_data
        optical = jnp.einsum("gs,lsc->lgc", coefficients, block_gas.astype(jnp.float32))
        heating, surface_down = layer_solve(optical, block_mass.astype(jnp.float32), block_state[0].astype(jnp.float32), block_state[1].astype(jnp.float32), single_scatter, solar_weight)
        heating = jnp.where(block_flag == 1, heating, jnp.zeros_like(heating))
        surface_down = jnp.where(block_flag == 1, surface_down, jnp.zeros_like(surface_down))
        return heating, surface_down

    heating, surface_down = lax.map(one_block, (gas_amounts, layer_mass, column_state, sunlit))
    return (heating, surface_down)
```

```python
import functools
import math

import jax
import jax.numpy as jnp
from jax import lax
from jax.experimental import pallas as pl
from jax.experimental.pallas import tpu as pltpu
from jax.sharding import PartitionSpec as P

LOG2E = 1.0 / math.log(2.0)


def gather_kernel(count, in_ref, out_ref, send_sem, recv_sem):
    me = lax.axis_index("sub")
    barrier = pltpu.get_barrier_semaphore()
    for step in range(1, count):
        pl.semaphore_signal(
            barrier,
            inc=1,
            device_id={"sub": lax.rem(me + step, count)},
            device_id_type=pl.DeviceIdType.MESH,
        )
    pl.semaphore_wait(barrier, count - 1)
    copies = []
    for step in range(1, count):
        copy = pltpu.make_async_remote_copy(
            src_ref=in_ref,
            dst_ref=out_ref.at[me],
            send_sem=send_sem.at[step - 1],
            recv_sem=recv_sem.at[step - 1],
            device_id={"sub": lax.rem(me + step, count)},
            device_id_type=pl.DeviceIdType.MESH,
        )
        copy.start()
        copies.append(copy)
    out_ref[pl.ds(me, 1)] = in_ref[...][None]
    for copy in copies:
        copy.wait()


def gather_tables(table, count):
    return pl.pallas_call(
        functools.partial(gather_kernel, count),
        out_shape=jax.ShapeDtypeStruct((count,) + table.shape, table.dtype),
        in_specs=[pl.BlockSpec(memory_space=pltpu.VMEM)],
        out_specs=pl.BlockSpec(memory_space=pltpu.VMEM),
        scratch_shapes=[
            pltpu.SemaphoreType.DMA((count - 1,)),
            pltpu.SemaphoreType.DMA((count - 1,)),
        ],
        compiler_params=pltpu.CompilerParams(collective_id=0, has_side_effects=True),
    )(table)


def solve_kernel(
    share, levels, gases, chunk, unroll,
    base_ref, flag_ref, gas_hbm, mass_hbm, state_hbm, coef_ref, omega_ref, weight_ref,
    heat_ref, down_ref,
    gas, mass, state, wide, half, weight, passing, direct, inverse, albedo, net, sems,
):
    gpoints, columns = half.shape
    base = base_ref[0]

    def fetch(j):
        return (
            pltpu.make_async_copy(gas_hbm.at[base + j], gas.at[j], sems.at[0, j]),
            pltpu.make_async_copy(mass_hbm.at[base + j], mass.at[j], sems.at[1, j]),
            pltpu.make_async_copy(state_hbm.at[base + j], state.at[j], sems.at[2, j]),
        )

    def start(j, carry):
        for copy in fetch(j):
            copy.start()
        return carry

    lax.fori_loop(0, share, start, 0)
    half[...] = jnp.broadcast_to(0.5 * omega_ref[...], half.shape)
    weight[...] = jnp.broadcast_to(weight_ref[...], weight.shape)
    lane = lax.broadcasted_iota(jnp.int32, (gpoints, chunk * gases), 1) // gases
    table = coef_ref[...].astype(jnp.float32)
    for i in range(chunk):
        wide[i * gpoints : (i + 1) * gpoints, :] = jnp.where(
            lane == chunk - 1 - i, table, 0.0
        ).astype(jnp.bfloat16)

    def solve(j, carry):
        for copy in fetch(j):
            copy.wait()

        @pl.when(flag_ref[j] == 1)
        def _():
            own = state[j].astype(jnp.float32)
            cosine = own[0:1, :]
            ground = own[1:2, :]
            scale = jnp.broadcast_to(1.0 / cosine, (8, columns))
            scale = jnp.concatenate([scale] * (gpoints // 8), axis=0)

            def upward(step, lower):
                first = levels - (step + 1) * chunk
                rows = gas[j, pl.ds(pl.multiple_of(first * gases, chunk * gases), chunk * gases), :]
                optical = jnp.dot(wide[...], rows, preferred_element_type=jnp.float32)
                for i in range(chunk):
                    layer = first + (chunk - 1 - i)
                    power = optical[i * gpoints : (i + 1) * gpoints] * (-LOG2E)
                    passed = jnp.exp2(power)
                    passing[layer] = passed
                    direct[layer] = jnp.exp2(power * scale)
                    squared = passed * passed
                    reflected = half[...] * (1.0 - squared)
                    rate = 1.0 / (1.0 - reflected * lower)
                    inverse[layer] = rate
                    lower = reflected + squared * (lower * rate)
                    albedo[layer] = lower
                return lower

            lax.fori_loop(
                0, levels // chunk, upward, jnp.broadcast_to(ground, (gpoints, columns))
            )

            def total(x):
                return jnp.sum(x.reshape(gpoints // 8, 8, columns), axis=0)

            def downward(step, carry):
                beam, diffuse = carry
                for i in range(unroll):
                    layer = step * unroll + i
                    net[layer] = total((1.0 - albedo[layer]) * (beam + diffuse))
                    after = beam * direct[layer]
                    diffuse = (
                        passing[layer] * diffuse + half[...] * (beam - after)
                    ) * inverse[layer]
                    beam = after
                return beam, diffuse

            beam, diffuse = lax.fori_loop(
                0,
                levels // unroll,
                downward,
                (weight[...] * cosine, jnp.zeros((gpoints, columns), jnp.float32)),
            )
            bottom = total(beam + diffuse)
            net[levels] = (1.0 - ground) * bottom
            change = jnp.sum(net[0:levels] - net[1 : levels + 1], axis=1)
            heat_ref[j] = mass[j].astype(jnp.float32) * change
            down_ref[pl.ds(j, 1), :] = jnp.sum(bottom, axis=0, keepdims=True)

        @pl.when(flag_ref[j] != 1)
        def _():
            heat_ref[j] = jnp.zeros((levels, columns), jnp.float32)
            down_ref[pl.ds(j, 1), :] = jnp.zeros((1, columns), jnp.float32)

        return carry

    lax.fori_loop(0, share, solve, 0)


def body(gas_amounts, layer_mass, column_state, absorption, single_scatter, solar_weight, sunlit):
    sub_count = lax.axis_size("sub")
    owned, levels, gases, columns = gas_amounts.shape
    share = owned // sub_count
    local = absorption.shape[0]
    gpoints = local * sub_count
    base = lax.axis_index("sub") * share
    flags = lax.dynamic_slice_in_dim(sunlit, lax.axis_index("band") * owned + base, share)
    table = jnp.concatenate(
        [
            absorption.astype(jnp.float32),
            single_scatter[:, None],
            solar_weight[:, None],
        ],
        axis=1,
    )
    table = jnp.pad(table, ((0, -local % 8), (0, 128 - gases - 2)))
    gathered = gather_tables(table, sub_count)[:, :local].reshape(gpoints, 128)
    chunk = 128 // gases
    coefficients = jnp.tile(gathered[:, :gases].astype(jnp.bfloat16), (1, chunk))
    omega = gathered[:, gases : gases + 1]
    weight = gathered[:, gases + 1 : gases + 2]
    smem = pl.BlockSpec(memory_space=pltpu.SMEM)
    vmem = pl.BlockSpec(memory_space=pltpu.VMEM)
    hbm = pl.BlockSpec(memory_space=pl.ANY)
    f32 = jnp.float32
    return pl.pallas_call(
        functools.partial(solve_kernel, share, levels, gases, chunk, 4),
        out_shape=(
            jax.ShapeDtypeStruct((share, levels, columns), f32),
            jax.ShapeDtypeStruct((share, columns), f32),
        ),
        in_specs=[smem, smem, hbm, hbm, hbm, vmem, vmem, vmem],
        out_specs=(vmem, vmem),
        scratch_shapes=[
            pltpu.VMEM((share, levels * gases, columns), jnp.bfloat16),
            pltpu.VMEM((share, levels, columns), jnp.bfloat16),
            pltpu.VMEM((share, 2, columns), jnp.bfloat16),
            pltpu.VMEM((chunk * gpoints, chunk * gases), jnp.bfloat16),
            pltpu.VMEM((gpoints, columns), f32),
            pltpu.VMEM((gpoints, columns), f32),
            pltpu.VMEM((levels, gpoints, columns), f32),
            pltpu.VMEM((levels, gpoints, columns), f32),
            pltpu.VMEM((levels, gpoints, columns), f32),
            pltpu.VMEM((levels, gpoints, columns), f32),
            pltpu.VMEM((levels + 1, 8, columns), f32),
            pltpu.SemaphoreType.DMA((3, share)),
        ],
        compiler_params=pltpu.CompilerParams(vmem_limit_bytes=48 * 1024 * 1024),
    )(
        base.reshape(1).astype(jnp.int32),
        flags,
        gas_amounts.reshape(owned, levels * gases, columns),
        layer_mass,
        column_state,
        coefficients,
        omega,
        weight,
    )


def solution(mesh):
    in_specs = (
        P("band", None, None, None),
        P("band", None, None),
        P("band", None, None),
        P("sub", None),
        P("sub"),
        P("sub"),
        P(),
    )
    out_specs = (P(("band", "sub"), None, None), P(("band", "sub"), None))
    return jax.shard_map(body, mesh=mesh, in_specs=in_specs, out_specs=out_specs, check_vma=False)
```

```python
import functools
import math

import jax
import jax.numpy as jnp
from jax import lax
from jax.experimental import pallas as pl
from jax.experimental.pallas import tpu as pltpu
from jax.sharding import PartitionSpec as P

LOG2E = 1.0 / math.log(2.0)


def gather_kernel(count, in_ref, out_ref, send_sem, recv_sem):
    me = lax.axis_index("sub")
    barrier = pltpu.get_barrier_semaphore()
    for step in range(1, count):
        pl.semaphore_signal(
            barrier,
            inc=1,
            device_id={"sub": lax.rem(me + step, count)},
            device_id_type=pl.DeviceIdType.MESH,
        )
    pl.semaphore_wait(barrier, count - 1)
    copies = []
    for step in range(1, count):
        copy = pltpu.make_async_remote_copy(
            src_ref=in_ref,
            dst_ref=out_ref.at[me],
            send_sem=send_sem.at[step - 1],
            recv_sem=recv_sem.at[step - 1],
            device_id={"sub": lax.rem(me + step, count)},
            device_id_type=pl.DeviceIdType.MESH,
        )
        copy.start()
        copies.append(copy)
    out_ref[pl.ds(me, 1)] = in_ref[...][None]
    for copy in copies:
        copy.wait()


def gather_tables(table, count):
    return pl.pallas_call(
        functools.partial(gather_kernel, count),
        out_shape=jax.ShapeDtypeStruct((count,) + table.shape, table.dtype),
        in_specs=[pl.BlockSpec(memory_space=pltpu.VMEM)],
        out_specs=pl.BlockSpec(memory_space=pltpu.VMEM),
        scratch_shapes=[
            pltpu.SemaphoreType.DMA((count - 1,)),
            pltpu.SemaphoreType.DMA((count - 1,)),
        ],
        compiler_params=pltpu.CompilerParams(collective_id=0, has_side_effects=True),
    )(table)


def solve_kernel(
    share, levels, gases, chunk, unroll,
    flag_ref, gas_hbm, mass_hbm, state_hbm, tables_ref,
    heat_ref, down_ref,
    gas, mass, state, table, wide, half, weight, passing, direct, inverse, albedo, net, sems,
):
    gpoints, columns = half.shape
    base = lax.axis_index("sub") * share
    first_flag = lax.axis_index("band") * gas_hbm.shape[0] + base

    def fetch(j):
        return (
            pltpu.make_async_copy(gas_hbm.at[base + j], gas.at[j], sems.at[0, j]),
            pltpu.make_async_copy(mass_hbm.at[base + j], mass.at[j], sems.at[1, j]),
            pltpu.make_async_copy(state_hbm.at[base + j], state.at[j], sems.at[2, j]),
        )

    def start(j, carry):
        for copy in fetch(j):
            copy.start()
        return carry

    lax.fori_loop(0, share, start, 0)
    subs, rows, lanes = tables_ref.shape
    local = gpoints // subs
    blank = jnp.zeros((lanes - rows, lanes), jnp.float32)
    for s in range(subs):
        turned = jnp.concatenate([tables_ref[s], blank], axis=0).T
        table[s * local : (s + 1) * local, :] = turned[:local]
    full = table[...]
    half[...] = jnp.broadcast_to(0.5 * full[:, gases : gases + 1], half.shape)
    weight[...] = jnp.broadcast_to(full[:, gases + 1 : gases + 2], weight.shape)
    lane = lax.broadcasted_iota(jnp.int32, (gpoints, lanes), 1)
    spread = jnp.where(lane < gases, full, 0.0)
    width = gases
    while width < lanes:
        spread = spread + pltpu.roll(spread, width, 1)
        width *= 2
    lane = lane // gases
    for i in range(chunk):
        wide[i * gpoints : (i + 1) * gpoints, :] = jnp.where(
            lane == chunk - 1 - i, spread, 0.0
        ).astype(jnp.bfloat16)

    def solve(j, carry):
        for copy in fetch(j):
            copy.wait()

        @pl.when(flag_ref[first_flag + j] == 1)
        def _():
            own = state[j].astype(jnp.float32)
            cosine = own[0:1, :]
            ground = own[1:2, :]
            scale = jnp.broadcast_to(1.0 / cosine, (8, columns))
            scale = jnp.concatenate([scale] * (gpoints // 8), axis=0)

            def upward(step, lower):
                first = levels - (step + 1) * chunk
                rows = gas[j, pl.ds(pl.multiple_of(first * gases, chunk * gases), chunk * gases), :]
                optical = jnp.dot(wide[...], rows, preferred_element_type=jnp.float32)
                for i in range(chunk):
                    layer = first + (chunk - 1 - i)
                    power = optical[i * gpoints : (i + 1) * gpoints] * (-LOG2E)
                    passed = jnp.exp2(power)
                    passing[layer] = passed
                    direct[layer] = jnp.exp2(power * scale)
                    squared = passed * passed
                    reflected = half[...] * (1.0 - squared)
                    rate = 1.0 / (1.0 - reflected * lower)
                    inverse[layer] = rate
                    lower = reflected + squared * (lower * rate)
                    albedo[layer] = lower
                return lower

            lax.fori_loop(
                0, levels // chunk, upward, jnp.broadcast_to(ground, (gpoints, columns))
            )

            def total(x):
                return jnp.sum(x.reshape(gpoints // 8, 8, columns), axis=0)

            def downward(step, carry):
                beam, diffuse = carry
                for i in range(unroll):
                    layer = step * unroll + i
                    net[layer] = total((1.0 - albedo[layer]) * (beam + diffuse))
                    after = beam * direct[layer]
                    diffuse = (
                        passing[layer] * diffuse + half[...] * (beam - after)
                    ) * inverse[layer]
                    beam = after
                return beam, diffuse

            beam, diffuse = lax.fori_loop(
                0,
                levels // unroll,
                downward,
                (weight[...] * cosine, jnp.zeros((gpoints, columns), jnp.float32)),
            )
            bottom = total(beam + diffuse)
            net[levels] = (1.0 - ground) * bottom
            change = jnp.sum(net[0:levels] - net[1 : levels + 1], axis=1)
            heat_ref[j] = mass[j].astype(jnp.float32) * change
            down_ref[pl.ds(j, 1), :] = jnp.sum(bottom, axis=0, keepdims=True)

        @pl.when(flag_ref[first_flag + j] != 1)
        def _():
            heat_ref[j] = jnp.zeros((levels, columns), jnp.float32)
            down_ref[pl.ds(j, 1), :] = jnp.zeros((1, columns), jnp.float32)

        return carry

    lax.fori_loop(0, share, solve, 0)


def body(gas_amounts, layer_mass, column_state, absorption, single_scatter, solar_weight, sunlit):
    sub_count = lax.axis_size("sub")
    owned, levels, gases, columns = gas_amounts.shape
    share = owned // sub_count
    local = absorption.shape[0]
    gpoints = local * sub_count
    table = jnp.concatenate(
        [
            absorption.T.astype(jnp.float32),
            single_scatter[None, :],
            solar_weight[None, :],
        ],
        axis=0,
    )
    table = jnp.pad(table, ((0, -(gases + 2) % 8), (0, 128 - local)))
    gathered = gather_tables(table, sub_count)
    chunk = 128 // gases
    smem = pl.BlockSpec(memory_space=pltpu.SMEM)
    vmem = pl.BlockSpec(memory_space=pltpu.VMEM)
    hbm = pl.BlockSpec(memory_space=pltpu.HBM)
    f32 = jnp.float32
    return pl.pallas_call(
        functools.partial(solve_kernel, share, levels, gases, chunk, 4),
        out_shape=(
            jax.ShapeDtypeStruct((share, levels, columns), f32),
            jax.ShapeDtypeStruct((share, columns), f32),
        ),
        in_specs=[smem, hbm, hbm, hbm, vmem],
        out_specs=(vmem, vmem),
        scratch_shapes=[
            pltpu.VMEM((share, levels * gases, columns), jnp.bfloat16),
            pltpu.VMEM((share, levels, columns), jnp.bfloat16),
            pltpu.VMEM((share, 2, columns), jnp.bfloat16),
            pltpu.VMEM((gpoints, 128), f32),
            pltpu.VMEM((chunk * gpoints, chunk * gases), jnp.bfloat16),
            pltpu.VMEM((gpoints, columns), f32),
            pltpu.VMEM((gpoints, columns), f32),
            pltpu.VMEM((levels, gpoints, columns), f32),
            pltpu.VMEM((levels, gpoints, columns), f32),
            pltpu.VMEM((levels, gpoints, columns), f32),
            pltpu.VMEM((levels, gpoints, columns), f32),
            pltpu.VMEM((levels + 1, 8, columns), f32),
            pltpu.SemaphoreType.DMA((3, share)),
        ],
        compiler_params=pltpu.CompilerParams(vmem_limit_bytes=66000000),
    )(
        sunlit,
        gas_amounts.reshape(owned, levels * gases, columns),
        layer_mass,
        column_state,
        gathered,
    )


def solution(mesh):
    in_specs = (
        P("band", None, None, None),
        P("band", None, None),
        P("band", None, None),
        P("sub", None),
        P("sub"),
        P("sub"),
        P(),
    )
    out_specs = (P(("band", "sub"), None, None), P(("band", "sub"), None))
    return jax.shard_map(body, mesh=mesh, in_specs=in_specs, out_specs=out_specs, check_vma=False)
```
